128 devices in a mesh: path: 32 (over z_hi, y, x), tm: 4 (over z_lo, core).
Axes of the slice: x: 4, y: 4, z: 4 (z_hi: 2, z_lo: 2; z = z_hi * 2 + z_lo), core: 2. Of those that a mesh axis runs over, the one named last changes fastest.
Arguments:
- increments: bfloat16 [32768, 32, 1000], P(('path', 'tm')), may hold values from -6 to 6
- level_table: int32 [16384], replicated, may hold values from 0 to 4, as said below
- time_table: int32 [16384], replicated, may hold values from 0 to 31, as said below
Outputs:
- value_est: float32 [32], P('tm')
- grad_est: float32 [32, 1000], P('tm')
The draws below stay inside these ranges and needn't reach their ends.
Inputs may be any that keep to these rules, and one draw needn't show every extreme that they name: `level_table`: never falls from one block to the next. `time_table`: split the 32 time points into as many runs of consecutive points as the tm axis has devices; the 128 consecutive entries of each device fall equally into every run.
All inputs are finite; a program needn't handle non-finite values.
Results may differ from the reference program's by a relative error of at most 0.0003.
The reference program's roundings to bfloat16 on the way count: a program that leaves them out, or rounds other values in their place, can miss the bound.
Values may be sent and summed in bfloat16 or wider, within the bound.
A program may use at most 128 MiB of HBM per device.

```python
import jax
import jax.numpy as jnp
from jax import lax

D = 1000
K = 32
LEVELS = 5
BLOCK = 2
BLK_DEV = 128
BLOCKS = 16384
PATHS = 32768
N_PATH = 32
N_TM = 4


def draw_level_table(key, part):
    drawn = jax.random.randint(jax.random.fold_in(key, 11), (BLOCKS,), 0, LEVELS, dtype=jnp.int32)
    return jnp.sort(drawn)


def draw_time_table(key, part):
    devices = BLOCKS // BLK_DEV
    group_len = K // N_TM
    base = jnp.repeat(jnp.arange(N_TM, dtype=jnp.int32), BLK_DEV // N_TM)
    dev_keys = jax.random.split(jax.random.fold_in(key, 23), devices)
    shuffled = jax.vmap(lambda one_key: jax.random.permutation(one_key, base))(dev_keys)
    inside = jax.random.randint(jax.random.fold_in(key, 37), (devices, BLK_DEV), 0, group_len, dtype=jnp.int32)
    return (shuffled * group_len + inside).reshape(BLOCKS)


def shard_levels(stream_key, shape, pieces, smallest, top_value):
    loudness, own = 1.0, jax.random.fold_in(stream_key, 6)
    for dim, shards_of in pieces:
        steps = jnp.exp(jax.random.uniform(jax.random.fold_in(own, dim), (shards_of,), jnp.float32, smallest / len(pieces), top_value / len(pieces)))
        loudness = loudness * jnp.repeat(steps, shape[dim] // shards_of).reshape([-1 if axis == dim else 1 for axis in range(len(shape))])
    return loudness


def normal_values(rng, dims, scale, most, shards=(), kind=jnp.bfloat16):
    gain = shard_levels(rng, dims, shards, -0.22, 0.18) if shards else 1.0
    values = jax.random.normal(rng, dims, jnp.float32) * scale * gain
    return jnp.minimum(jnp.maximum(values, -most), most).astype(kind)


def setup_inputs(seed: int = 0) -> dict:
    arg_keys = jax.random.split(jax.random.key(seed), 4)
    increments = normal_values(arg_keys[0], (PATHS, K, D), 1.0, 6.0, ((0, 128),))
    level_table = draw_level_table(jax.random.fold_in(arg_keys[3], 71), 0)
    time_table = draw_time_table(jax.random.fold_in(arg_keys[3], 71), 0)
    return dict(increments=increments, level_table=level_table, time_table=time_table)


horizon = 0.3

def stride_weights(levels, starts, steps_k, step_len):
    steps = jnp.arange(steps_k).astype(jnp.int32)
    fine_stride = jnp.power(2, LEVELS - 1 - levels).astype(jnp.int32)
    coarse = fine_stride * 2
    live_steps = steps[None, :] >= starts[:, None]
    on_fine = steps[None, :] % fine_stride[:, None] == 0
    on_coarse = (steps[None, :] % coarse[:, None] == 0) & (levels[:, None] > 0)
    term = fine_stride[:, None] * on_fine.astype(jnp.int32) - coarse[:, None] * on_coarse.astype(jnp.int32)
    return step_len * (live_steps.astype(jnp.float32) * term.astype(jnp.float32))

def terminal(incr, starts):
    steps_k = incr.shape[1]
    width = incr.shape[2]
    step_len = horizon / steps_k
    steps = jnp.arange(steps_k).astype(jnp.int32)
    live_steps = (steps[None, :] >= starts[:, None]).astype(jnp.float32)
    end_point = jnp.sqrt(step_len) * jnp.einsum('pi,pid->pd', live_steps, incr.astype(jnp.float32), precision=lax.Precision.HIGHEST)
    remaining = horizon - starts.astype(jnp.float32) * step_len
    scaled = end_point / remaining[:, None]
    end_value = 1.0 / (2.0 + 0.4 * lax.optimization_barrier(jnp.sum(end_point * end_point, axis=1)) / width)
    return (scaled, end_value)

def partial_sums(path_total, scaled, row_index, path_share, row_count):
    select = (row_index[:, None] == jnp.arange(row_count).astype(jnp.int32)[None, :]).astype(jnp.float32)
    select = select * (path_share * path_total)[:, None]
    return (lax.optimization_barrier(jnp.sum(select, axis=0)), jnp.dot(select.T, scaled, precision=lax.Precision.HIGHEST))

def first_terms(incr, levels, starts, path_share, row_count, offset):
    scaled, end_value = terminal(incr, starts)
    path_total = end_value * (levels == 0).astype(jnp.float32)
    return partial_sums(path_total, scaled, starts - offset, path_share, row_count)

def second_terms(incr, levels, starts, path_share, value_one, grad_low, row_count, offset):
    paths, steps_k, width = incr.shape
    step_len = horizon / steps_k
    scaled, end_value = terminal(incr, starts)
    inner_dots = jnp.dot(incr.reshape(paths * steps_k, width), grad_low.T, preferred_element_type=jnp.float32).reshape(paths, steps_k, steps_k)
    steps = jnp.arange(steps_k).astype(jnp.int32)
    window = (steps[None, :, None] >= starts[:, None, None]) & (steps[None, :, None] < steps[None, None, :])
    estimate = value_one[None, :] + jnp.sqrt(step_len) * lax.optimization_barrier(jnp.sum(inner_dots * window.astype(jnp.float32), axis=1))
    drift_term = estimate - estimate * estimate * estimate
    weights = stride_weights(levels, starts, steps_k, step_len)
    path_total = end_value * (levels == 0).astype(jnp.float32) + lax.optimization_barrier(jnp.sum(weights * drift_term, axis=1))
    return partial_sums(path_total, scaled, starts - offset, path_share, row_count)

def reference(increments, level_table, time_table):
    steps_k = increments.shape[1]
    width = increments.shape[2]
    devices = N_PATH * N_TM
    lvl_hot = (level_table[:, None] == jnp.arange(LEVELS).astype(jnp.int32)[None, :]).astype(jnp.float32)
    time_hot = (time_table[:, None] == jnp.arange(steps_k).astype(jnp.int32)[None, :]).astype(jnp.float32)
    counts = jnp.dot(lvl_hot.T, time_hot, precision=lax.Precision.HIGHEST)
    lvl_path = jnp.repeat(level_table, BLOCK)
    time_path = jnp.repeat(time_table, BLOCK)
    path_share = 1.0 / (BLOCK * counts[lvl_path, time_path])
    inc_groups = increments.reshape(devices, -1, steps_k, width)
    lvl_groups = lvl_path.reshape(devices, -1)
    time_groups = time_path.reshape(devices, -1)
    share_groups = path_share.reshape(devices, -1)
    first_v, first_z = lax.map(lambda item: first_terms(item[0], item[1], item[2], item[3], steps_k, 0), (inc_groups, lvl_groups, time_groups, share_groups))
    value_one = lax.optimization_barrier(jnp.sum(first_v, axis=0))
    grad_one = lax.optimization_barrier(jnp.sum(first_z, axis=0))
    grad_low = grad_one.astype(jnp.bfloat16)
    second_v, second_z = lax.map(lambda item: second_terms(item[0], item[1], item[2], item[3], value_one, grad_low, steps_k, 0), (inc_groups, lvl_groups, time_groups, share_groups))
    return (lax.optimization_barrier(jnp.sum(second_v, axis=0)), lax.optimization_barrier(jnp.sum(second_z, axis=0)))
```

```python
import functools
import itertools

import jax
import jax.numpy as jnp
from jax import lax
from jax.experimental import pallas as pl
from jax.experimental.pallas import tpu as pltpu
from jax.sharding import PartitionSpec as P

LEVELS = 5
HORIZON = 0.3
MESH = pl.DeviceIdType.MESH
HIGHEST = lax.Precision.HIGHEST
SIDE = 4
GROUPS = (8, 8, 8, 4, 2, 2)


def reach(offset):
    return sum(min(d, SIDE - d) for d in offset)


def opposite(offset):
    return tuple((d + 2) % SIDE for d in offset)


def near(offset):
    other = opposite(offset)
    return (reach(offset), offset) < (reach(other), other)


OFFSETS = sorted(itertools.product(range(SIDE), repeat=3), key=lambda o: -reach(o))
NEAR = [o for o in OFFSETS if near(o)]
NEAR_PATH = [o for o in NEAR if o[0] % 2 == 0]


class Place:
    def __init__(self):
        self.path, self.tm = lax.axis_index("path"), lax.axis_index("tm")
        self.me = self.path * 4 + self.tm
        z_hi, y, x = self.path // 16, lax.rem(self.path // 4, 4), lax.rem(self.path, 4)
        z, core = z_hi * 2 + self.tm // 2, lax.rem(self.tm, 2)
        zs = [lax.rem(z + d, SIDE) for d in range(SIDE)]
        ys = [lax.rem(y + d, SIDE) for d in range(SIDE)]
        xs = [lax.rem(x + d, SIDE) for d in range(SIDE)]
        self.high = [q // 2 for q in zs]
        self.low = [lax.rem(q, 2) * 2 for q in zs]
        self.ys, self.xs = ys, xs
        self.cores = [core, 1 - core]
        turned_y = [lax.rem(q + 2, SIDE) for q in ys]
        turned_x = [lax.rem(q + 2, SIDE) for q in xs]
        self.turned_y, self.turned_x = turned_y, turned_x

    def peer(self, offset, core):
        dz, dy, dx = offset
        return (self.high[dz] * 16 + self.ys[dy] * 4 + self.xs[dx], self.low[dz] + self.cores[core])

    def piece(self, offset):
        dz, dy, dx = offset
        high = self.high[dz]
        at_y = self.ys[dy] + high * (self.turned_y[dy] - self.ys[dy])
        at_x = self.xs[dx] + high * (self.turned_x[dx] - self.xs[dx])
        return at_y * 4 + at_x

    def peers(self, offsets, cores=(0, 1)):
        for offset in offsets:
            for core in cores:
                if offset != (0, 0, 0) or core:
                    yield offset, self.peer(offset, core)


def wait_all(count, ref, sem, place, sent):
    window = ref.at[pl.ds(0, count)]
    copy = pltpu.make_async_remote_copy(
        src_ref=window, dst_ref=window, send_sem=sem, recv_sem=sem,
        device_id=(place.path, place.tm), device_id_type=MESH,
    )
    if sent:
        copy.wait_send()
    else:
        copy.wait_recv()


def kernel(
    inc_hbm, lvl_ref, time_ref, value_ref, grad_ref,
    inc, end, mask, whole, mine, scattered, arrived, total, gathered,
    load_sem, scatter_send, scatter_recv, gather_send, gather_recv,
):
    steps_k, width, paths = inc.shape
    step_len = HORIZON / steps_k
    root = jnp.sqrt(jnp.float32(step_len))
    place = Place()
    devices = 128

    loads = [pltpu.make_async_copy(inc_hbm.at[i], inc.at[i], load_sem.at[i]) for i in range(steps_k)]
    for load in loads:
        load.start()
    barrier = pltpu.get_barrier_semaphore()
    for _, peer in place.peers(OFFSETS):
        pl.semaphore_signal(barrier, inc=1, device_id=peer, device_id_type=MESH)

    row_of = lax.broadcasted_iota(jnp.int32, (8, 128), 0)
    own_lvl = lvl_ref[pl.ds(place.me, 1), :].astype(jnp.float32)
    own_time = time_ref[pl.ds(place.me, 1), :].astype(jnp.float32)
    both = jnp.where(row_of == 0, own_lvl, own_time).astype(jnp.bfloat16)
    spread = (
        lax.broadcasted_iota(jnp.int32, (128, paths), 1) // 2
        == lax.broadcasted_iota(jnp.int32, (128, paths), 0)
    ).astype(jnp.float32).astype(jnp.bfloat16)
    per_path = jnp.dot(both, spread, preferred_element_type=jnp.float32)
    lvl, start = per_path[0:1], per_path[1:2]
    start_16 = jnp.broadcast_to(start, (16, paths))
    for i in range(steps_k):
        mask[i] = jnp.where(start_16 <= i, 1.0, 0.0).astype(jnp.bfloat16)

    step_row = lax.broadcasted_iota(jnp.int32, (steps_k, 128), 0)
    counts = [jnp.zeros((steps_k, 128), jnp.int32) for _ in range(LEVELS)]
    for part in range(4):
        packed = jnp.zeros((steps_k, 128), jnp.int32)
        for r in range(part * 32, part * 32 + 32):
            unit = jnp.left_shift(jnp.int32(1), 6 * lvl_ref[pl.ds(r, 1), :])
            packed = packed + jnp.where(time_ref[pl.ds(r, 1), :] == step_row, unit, 0)
        counts = [c + (jnp.right_shift(packed, 6 * n) & 63) for n, c in enumerate(counts)]
    shares = [
        1.0 / (2.0 * jnp.sum(c.astype(jnp.float32), axis=1, keepdims=True)) for c in counts
    ]
    step_at = lax.broadcasted_iota(jnp.int32, (steps_k, paths), 0)
    step_f = step_at.astype(jnp.float32)
    share = jnp.broadcast_to(shares[-1], (steps_k, paths))
    for n in range(LEVELS - 1):
        share = jnp.where(lvl == n, shares[n], share)
    share = jnp.where(start == step_f, share, 0.0)
    scale = root / (HORIZON - step_f[:, 0:1] * step_len)

    first_slab = 0
    for size in GROUPS:
        slabs = range(first_slab, first_slab + size)
        for i in slabs:
            loads[i].wait()
        masks = [mask[i] for i in slabs]

        def add(at, rows, slabs=slabs, masks=masks):
            terms = [
                (inc[i, pl.ds(at, rows), :] * jnp.concatenate([m] * (rows // 16), axis=0) if rows >= 16
                 else inc[i, pl.ds(at, rows), :] * m[0:rows]).astype(jnp.float32)
                for i, m in zip(slabs, masks)
            ]
            while len(terms) > 1:
                terms = [a + b for a, b in zip(terms[::2], terms[1::2])]
            if slabs[0]:
                end[pl.ds(at, rows), :] += terms[0]
            else:
                end[pl.ds(at, rows), :] = terms[0]

        @pl.loop(0, width // 32)
        def _(n):
            add(pl.multiple_of(n * 32, 32), 32)

        add(width // 32 * 32, width % 32)
        first_slab += size
    end[pl.ds(width, end.shape[0] - width), :] = jnp.zeros((end.shape[0] - width, paths), jnp.float32)

    ends = end[...]
    scaled = root * ends
    norm = jnp.sum(scaled * scaled, axis=0, keepdims=True)
    end_value = 1.0 / (2.0 + 0.4 * norm / width)
    first = jnp.where(lvl == 0.0, end_value, 0.0)

    def partial_sums(path_total, at):
        select = share * path_total
        grads = lax.dot_general(
            select * scale, end[...], (((1,), (1,)), ((), ())),
            precision=HIGHEST, preferred_element_type=jnp.float32,
        )
        values = jnp.sum(select, axis=1, keepdims=True)
        column = lax.broadcasted_iota(jnp.int32, grads.shape, 1)
        grads = jnp.where(column == width, values, grads)
        for t, c, r in itertools.product(range(4), range(8), range(2)):
            mine[at, t * 16 + c * 2 + r] = grads[8 * t + 4 * r : 8 * t + 4 * r + 4, 128 * c : 128 * c + 128]

    def scatter(at):
        for offset, (path, tm) in place.peers(OFFSETS):
            pltpu.make_async_remote_copy(
                src_ref=mine.at[at, tm * 16 + place.piece(offset)], dst_ref=scattered.at[at, place.me],
                send_sem=scatter_send.at[at], recv_sem=scatter_recv.at[at],
                device_id=(path, tm), device_id_type=MESH,
            ).start()
        scattered[at, place.me] = mine[at, place.tm * 16 + place.piece((0, 0, 0))]

    def added(at):
        wait_all(devices - 1, scattered.at[at], scatter_recv.at[at], place, False)
        return jnp.sum(scattered[at], axis=0)

    def gather(at, subtotal, offsets, cores, slot, home):
        total[at] = subtotal
        peers = list(place.peers(offsets, cores))
        for _, peer in peers:
            pltpu.make_async_remote_copy(
                src_ref=total.at[at], dst_ref=home.at[slot],
                send_sem=gather_send.at[at], recv_sem=gather_recv.at[at],
                device_id=peer, device_id_type=MESH,
            ).start()
        home[slot] = subtotal
        wait_all(len(peers), home, gather_recv.at[at], place, False)
        return len(peers)

    partial_sums(first, 0)
    pl.semaphore_wait(barrier, devices - 1)
    scatter(0)

    fine = jnp.where(lvl == 0.0, 16, jnp.where(lvl == 1.0, 8, jnp.where(lvl == 2.0, 4, jnp.where(lvl == 3.0, 2, 1))))
    on_fine = (step_at & (fine - 1)) == 0
    on_coarse = ((step_at & (2 * fine - 1)) == 0) & (lvl > 0.0)
    fine_f = fine.astype(jnp.float32)
    weight = step_len * (jnp.where(on_fine, fine_f, 0.0) - jnp.where(on_coarse, 2.0 * fine_f, 0.0))
    weight = jnp.where(step_f >= start, weight, 0.0)

    own = place.piece((0, 0, 0))
    sent = gather(0, added(0), NEAR, (0, 1), place.tm * 16 + own, arrived)
    for t, c, r in itertools.product(range(4), range(8), range(2)):
        whole[8 * t + 4 * r : 8 * t + 4 * r + 4, 128 * c : 128 * c + 128] = arrived[t * 16 + c * 2 + r]
    value_one = whole[:, width : width + 1]
    grad_low = whole[:, 0:width].astype(jnp.bfloat16)

    inner = jnp.zeros((steps_k, paths), jnp.float32)
    for i in range(steps_k - 1):
        dots = jnp.dot(grad_low, inc[i], preferred_element_type=jnp.float32)
        inner = inner + jnp.where((start <= i) & (step_at > i), dots, 0.0)
    estimate = value_one + root * inner
    drift = estimate - estimate * estimate * estimate
    second = first + jnp.sum(weight * drift, axis=0, keepdims=True)
    partial_sums(second, 1)
    scatter(1)
    gather_one = sent
    sent = gather(1, added(1), NEAR_PATH, (0,), own, gathered)
    for c, r in itertools.product(range(8), range(2)):
        whole[4 * r : 4 * r + 4, 128 * c : 128 * c + 128] = gathered[c * 2 + r]
    out = whole[0:8, :]
    grad_ref[...] = out[:, 0:width]
    eye = lax.broadcasted_iota(jnp.int32, (8, 8), 0) == lax.broadcasted_iota(jnp.int32, (8, 8), 1)
    value_ref[...] = jnp.sum(jnp.where(eye, out[:, width : width + 1], 0.0), axis=0, keepdims=True)

    for at in range(2):
        wait_all(devices - 1, scattered.at[at], scatter_send.at[at], place, True)
    wait_all(gather_one, arrived, gather_send.at[0], place, True)
    wait_all(sent, gathered, gather_send.at[1], place, True)


def shards(increments, level_table, time_table):
    paths, steps_k, width = increments.shape
    slabs = jnp.transpose(increments, (1, 2, 0))
    value, grad = pl.pallas_call(
        kernel,
        out_shape=(
            jax.ShapeDtypeStruct((1, 8), jnp.float32),
            jax.ShapeDtypeStruct((8, width), jnp.float32),
        ),
        in_specs=[
            pl.BlockSpec(memory_space=pl.ANY),
            pl.BlockSpec(memory_space=pltpu.VMEM),
            pl.BlockSpec(memory_space=pltpu.VMEM),
        ],
        out_specs=(pl.BlockSpec(memory_space=pltpu.VMEM), pl.BlockSpec(memory_space=pltpu.VMEM)),
        scratch_shapes=[
            pltpu.VMEM((steps_k, width, paths), jnp.bfloat16),
            pltpu.VMEM((1024, paths), jnp.float32),
            pltpu.VMEM((steps_k, 16, paths), jnp.bfloat16),
            pltpu.VMEM((steps_k, 1024), jnp.float32),
            pltpu.VMEM((2, 64, 4, 128), jnp.float32),
            pltpu.VMEM((2, 128, 4, 128), jnp.float32),
            pltpu.VMEM((64, 4, 128), jnp.float32),
            pltpu.VMEM((2, 4, 128), jnp.float32),
            pltpu.VMEM((16, 4, 128), jnp.float32),
            pltpu.SemaphoreType.DMA((steps_k,)),
            pltpu.SemaphoreType.DMA((2,)),
            pltpu.SemaphoreType.DMA((2,)),
            pltpu.SemaphoreType.DMA((2,)),
            pltpu.SemaphoreType.DMA((2,)),
        ],
        compiler_params=pltpu.CompilerParams(
            collective_id=0, has_side_effects=True, vmem_limit_bytes=48 * 1024 * 1024
        ),
    )(slabs, level_table.reshape(128, 128), time_table.reshape(128, 128))
    return (value.reshape(8), grad)


def solution(mesh):
    placed = (P(("path", "tm"), None, None), P(), P())
    return jax.shard_map(
        shards, mesh=mesh, in_specs=placed, out_specs=(P("tm"), P("tm", None)), check_vma=False
    )
```

```python
import functools
import itertools

import jax
import jax.numpy as jnp
from jax import lax
from jax.experimental import pallas as pl
from jax.experimental.pallas import tpu as pltpu
from jax.sharding import PartitionSpec as P

LEVELS = 5
HORIZON = 0.3
MESH = pl.DeviceIdType.MESH
HIGHEST = lax.Precision.HIGHEST
SIDE = 4
GROUPS = (8, 8, 8, 4, 3, 1)
ROWS = 64


def reach(offset):
    return sum(min(d, SIDE - d) for d in offset)


def opposite(offset):
    return tuple((d + 2) % SIDE for d in offset)


def near(offset):
    other = opposite(offset)
    return (reach(offset), offset) < (reach(other), other)


OFFSETS = sorted(itertools.product(range(SIDE), repeat=3), key=lambda o: -reach(o))
NEAR = [o for o in OFFSETS if near(o)]
NEAR_BACK = [tuple((SIDE - d) % SIDE for d in o) for o in NEAR]
NEAR_PATH = [o for o in NEAR if o[0] % 2 == 0]


class Place:
    def __init__(self):
        self.path, self.tm = lax.axis_index("path"), lax.axis_index("tm")
        self.me = self.path * 4 + self.tm
        z_hi, y, x = self.path // 16, lax.rem(self.path // 4, 4), lax.rem(self.path, 4)
        z, core = z_hi * 2 + self.tm // 2, lax.rem(self.tm, 2)
        self.core, self.chip = core, self.me // 2
        side = range(SIDE)
        zs = [lax.rem(z + d, SIDE) for d in side]
        high = [q // 2 for q in zs]
        self.odd = [lax.rem(q, 2) for q in zs]
        low = [q * 2 for q in self.odd]
        self.zy = [[high[a] * 16 + lax.rem(y + b, SIDE) * 4 for b in side] for a in side]
        self.x = [lax.rem(x + d, SIDE) for d in side]
        self.tms = [[low[a] + core, low[a] + 1 - core] for a in side]
        self.piece_y = [[lax.rem(y + b + 2 * high[a], SIDE) * 4 for b in side] for a in side]
        self.piece_x = [[lax.rem(x + b + 2 * high[a], SIDE) for b in side] for a in side]

    def peer(self, offset, core):
        dz, dy, dx = offset
        return (self.zy[dz][dy] + self.x[dx], self.tms[dz][core])

    def piece(self, offset):
        dz, dy, dx = offset
        return self.piece_y[dz][dy] + self.piece_x[dz][dx]

    def peers(self, offsets, cores=(0, 1)):
        for offset in offsets:
            for core in cores:
                if offset != (0, 0, 0) or core:
                    yield offset, self.peer(offset, core)


def parts(array, count):
    found = []
    for _ in range(count):
        found.append(array.astype(jnp.bfloat16))
        array = array - found[-1].astype(jnp.float32)
    return found


def wait_all(count, ref, sem, place, sent):
    window = ref.at[pl.ds(0, count)]
    copy = pltpu.make_async_remote_copy(
        src_ref=window, dst_ref=window, send_sem=sem, recv_sem=sem,
        device_id=(place.path, place.tm), device_id_type=MESH,
    )
    if sent:
        copy.wait_send()
    else:
        copy.wait_recv()


def kernel(
    inc_hbm, lvl_hbm, time_hbm, value_ref, grad_ref,
    inc, lvl_ref, time_ref, end, end_parts, mask, whole, mine, paired, summed, scattered, arrived, total, gathered,
    table_sem, load_sem, pair_send, pair_recv, scatter_send, scatter_recv, gather_send, gather_recv,
):
    steps_k, width, paths = inc.shape
    step_len = HORIZON / steps_k
    root = jnp.sqrt(jnp.float32(step_len))
    place = Place()
    chips = SIDE**3

    tables = [
        pltpu.make_async_copy(lvl_hbm, lvl_ref, table_sem.at[0]),
        pltpu.make_async_copy(time_hbm, time_ref, table_sem.at[1]),
    ]
    for table in tables:
        table.start()
    loads = [pltpu.make_async_copy(inc_hbm.at[i], inc.at[i], load_sem.at[i]) for i in range(steps_k)]
    for load in loads:
        load.start(priority=1)
    barrier = pltpu.get_barrier_semaphore()
    senders = list(place.peers(OFFSETS, (0,))) + list(place.peers(NEAR_BACK, (1,)))
    for _, peer in senders:
        pl.semaphore_signal(barrier, inc=1, device_id=peer, device_id_type=MESH)

    for table in tables:
        table.wait()

    row_of = lax.broadcasted_iota(jnp.int32, (8, 128), 0)
    own_lvl = lvl_ref[pl.ds(place.me, 1), :].astype(jnp.float32)
    own_time = time_ref[pl.ds(place.me, 1), :].astype(jnp.float32)
    both = jnp.where(row_of == 0, own_lvl, own_time).astype(jnp.bfloat16)
    spread = (
        lax.broadcasted_iota(jnp.int32, (128, paths), 1) // 2
        == lax.broadcasted_iota(jnp.int32, (128, paths), 0)
    ).astype(jnp.float32).astype(jnp.bfloat16)
    per_path = jnp.dot(both, spread, preferred_element_type=jnp.float32)
    lvl, start = per_path[0:1], per_path[1:2]
    start_16 = jnp.broadcast_to(start, (16, paths))
    for i in range(steps_k):
        mask[i] = jnp.where(start_16 <= i, 1.0, 0.0).astype(jnp.bfloat16)

    step_row = lax.broadcasted_iota(jnp.int32, (steps_k, 128), 0)
    counts = [jnp.zeros((steps_k, 128), jnp.int32) for _ in range(LEVELS)]
    for part in range(4):
        packed = jnp.zeros((steps_k, 128), jnp.int32)
        for r in range(part * 32, part * 32 + 32):
            unit = jnp.left_shift(jnp.int32(1), 6 * lvl_ref[pl.ds(r, 1), :])
            packed = packed + jnp.where(time_ref[pl.ds(r, 1), :] == step_row, unit, 0)
        counts = [c + (jnp.right_shift(packed, 6 * n) & 63) for n, c in enumerate(counts)]
    shares = [
        1.0 / (2.0 * jnp.sum(c.astype(jnp.float32), axis=1, keepdims=True)) for c in counts
    ]
    padding = end_parts.shape[1] - width
    end_parts[:, pl.ds(width, padding), :] = jnp.zeros((3, padding, paths), jnp.bfloat16)
    step_at = lax.broadcasted_iota(jnp.int32, (steps_k, paths), 0)
    step_f = step_at.astype(jnp.float32)
    share = jnp.broadcast_to(shares[-1], (steps_k, paths))
    for n in range(LEVELS - 1):
        share = jnp.where(lvl == n, shares[n], share)
    share = jnp.where(start == step_f, share, 0.0)
    scale = root / (HORIZON - step_f[:, 0:1] * step_len)

    def masked_sum(at, rows, slabs, masks):
        terms = []
        for i, m in zip(slabs, masks):
            tiles = [m] * (rows // 16) + ([m[0 : rows % 16]] if rows % 16 else [])
            live = tiles[0] if len(tiles) == 1 else jnp.concatenate(tiles, axis=0)
            terms.append((inc[i, pl.ds(at, rows), :] * live).astype(jnp.float32))
        while len(terms) > 1:
            terms = [sum(terms[n : n + 2][1:], terms[n]) for n in range(0, len(terms), 2)]
        return terms[0]

    chunks, rest = width // ROWS, width % ROWS
    first_slab = 0
    for size in GROUPS[:-1]:
        slabs = range(first_slab, first_slab + size)
        for i in slabs:
            loads[i].wait()
        masks = [mask[i] for i in slabs]

        def add(at, rows, slabs=slabs, masks=masks):
            total_here = masked_sum(at, rows, slabs, masks)
            if slabs[0]:
                end[pl.ds(at, rows), :] += total_here
            else:
                end[pl.ds(at, rows), :] = total_here

        @pl.loop(0, chunks)
        def _(n):
            add(pl.multiple_of(n * ROWS, ROWS), ROWS)

        add(chunks * ROWS, rest)
        first_slab += size

    slabs = range(first_slab, steps_k)
    for i in slabs:
        loads[i].wait()
    masks = [mask[i] for i in slabs]

    def finish(at, rows, squares):
        ended = end[pl.ds(at, rows), :] + masked_sum(at, rows, slabs, masks)
        for n, part in enumerate(parts(ended, 3)):
            end_parts[n, pl.ds(at, rows), :] = part
        return squares + jnp.sum((ended * ended).reshape(rows // 8, 8, paths), axis=0)

    squares = lax.fori_loop(
        0, chunks, lambda n, c: finish(pl.multiple_of(n * ROWS, ROWS), ROWS, c), jnp.zeros((8, paths), jnp.float32)
    )
    squares = finish(chunks * ROWS, rest, squares)
    norm = step_len * jnp.sum(squares, axis=0, keepdims=True)
    end_value = 1.0 / (2.0 + 0.4 * norm / width)
    first = jnp.where(lvl == 0.0, end_value, 0.0)

    def partial_sums(path_total, at, depth):
        select = share * path_total
        weights = parts(select * scale, depth)
        products = []
        for n in range(depth):
            found = lax.dot_general(
                jnp.concatenate(weights[: depth - n], axis=0), end_parts[n],
                (((1,), (1,)), ((), ())), preferred_element_type=jnp.float32,
            )
            products += [(n + m, found[m * steps_k : (m + 1) * steps_k]) for m in range(depth - n)]
        products.sort(key=lambda pair: -pair[0])
        grads = products[0][1]
        for _, product in products[1:]:
            grads = grads + product
        values = jnp.sum(select, axis=1, keepdims=True)
        lane = lax.broadcasted_iota(jnp.int32, (steps_k, 128), 1)
        for c in range(8):
            tile = grads[:, 128 * c : 128 * c + 128]
            if c == width // 128:
                tile = jnp.where(lane == width % 128, values, tile)
            for t, r in itertools.product(range(4), range(2)):
                mine[at, t * 16 + c * 2 + r] = tile[8 * t + 4 * r : 8 * t + 4 * r + 4]

    def scatter(at):
        partner = place.peer((0, 0, 0), 1)
        for k in range(2):
            pltpu.make_async_remote_copy(
                src_ref=mine.at[at, pl.ds((2 * k + 1 - place.core) * 16, 16)], dst_ref=paired.at[at, pl.ds(k * 16, 16)],
                send_sem=pair_send.at[at], recv_sem=pair_recv.at[at],
                device_id=partner, device_id_type=MESH,
            ).start()
        wait_all(32, paired.at[at], pair_recv.at[at], place, False)
        for k in range(2):
            summed[at, pl.ds(k * 16, 16)] = (
                mine[at, pl.ds((2 * k + place.core) * 16, 16)] + paired[at, pl.ds(k * 16, 16)]
            )
        for offset, peer in place.peers(OFFSETS, (0,)):
            pltpu.make_async_remote_copy(
                src_ref=summed.at[at, place.odd[offset[0]] * 16 + place.piece(offset)],
                dst_ref=scattered.at[at, place.chip],
                send_sem=scatter_send.at[at], recv_sem=scatter_recv.at[at],
                device_id=peer, device_id_type=MESH,
            ).start()
        scattered[at, place.chip] = summed[at, place.odd[0] * 16 + place.piece((0, 0, 0))]

    def added(at):
        wait_all(chips - 1, scattered.at[at], scatter_recv.at[at], place, False)
        terms = [scattered[at, n] for n in range(chips)]
        while len(terms) > 1:
            terms = [a + b for a, b in zip(terms[::2], terms[1::2])]
        return terms[0]

    def gather(at, subtotal, offsets, cores, slot, home):
        total[at] = subtotal
        peers = list(place.peers(offsets, cores))
        for _, peer in peers:
            pltpu.make_async_remote_copy(
                src_ref=total.at[at], dst_ref=home.at[slot],
                send_sem=gather_send.at[at], recv_sem=gather_recv.at[at],
                device_id=peer, device_id_type=MESH,
            ).start()
        home[slot] = subtotal
        wait_all(len(peers), home, gather_recv.at[at], place, False)
        return len(peers)

    partial_sums(first, 0, 3)
    pl.semaphore_wait(barrier, len(senders))
    scatter(0)

    fine = jnp.where(lvl == 0.0, 16, jnp.where(lvl == 1.0, 8, jnp.where(lvl == 2.0, 4, jnp.where(lvl == 3.0, 2, 1))))
    on_fine = (step_at & (fine - 1)) == 0
    on_coarse = ((step_at & (2 * fine - 1)) == 0) & (lvl > 0.0)
    fine_f = fine.astype(jnp.float32)
    weight = step_len * (jnp.where(on_fine, fine_f, 0.0) - jnp.where(on_coarse, 2.0 * fine_f, 0.0))
    weight = jnp.where(step_f >= start, weight, 0.0)

    own = place.piece((0, 0, 0))
    sent = gather(0, added(0), NEAR, (0, 1), place.tm * 16 + own, arrived)
    for t, c, r in itertools.product(range(4), range(8), range(2)):
        whole[8 * t + 4 * r : 8 * t + 4 * r + 4, 128 * c : 128 * c + 128] = arrived[t * 16 + c * 2 + r]
    value_one = whole[:, width : width + 1]
    grad_low = whole[:, 0:width].astype(jnp.bfloat16)

    inner = jnp.zeros((steps_k, paths), jnp.float32)
    for i in range(steps_k - 1):
        dots = jnp.dot(grad_low, inc[i], preferred_element_type=jnp.float32)
        inner = inner + jnp.where((start <= i) & (step_at > i), dots, 0.0)
    estimate = value_one + root * inner
    drift = estimate - estimate * estimate * estimate
    second = first + jnp.sum(weight * drift, axis=0, keepdims=True)
    partial_sums(second, 1, 2)
    scatter(1)
    gather_one = sent
    sent = gather(1, added(1), NEAR_PATH, (0,), own, gathered)
    for c, r in itertools.product(range(8), range(2)):
        whole[4 * r : 4 * r + 4, 128 * c : 128 * c + 128] = gathered[c * 2 + r]
    out = whole[0:8, :]
    grad_ref[...] = out[:, 0:width]
    eye = lax.broadcasted_iota(jnp.int32, (8, 8), 0) == lax.broadcasted_iota(jnp.int32, (8, 8), 1)
    value_ref[...] = jnp.sum(jnp.where(eye, out[:, width : width + 1], 0.0), axis=0, keepdims=True)

    for at in range(2):
        wait_all(32, paired.at[at], pair_send.at[at], place, True)
        wait_all(chips - 1, scattered.at[at], scatter_send.at[at], place, True)
    wait_all(gather_one, arrived, gather_send.at[0], place, True)
    wait_all(sent, gathered, gather_send.at[1], place, True)


def shards(increments, level_table, time_table):
    paths, steps_k, width = increments.shape
    slabs = jnp.transpose(increments, (1, 2, 0))
    value, grad = pl.pallas_call(
        kernel,
        out_shape=(
            pltpu.VMEM((1, 8), jnp.float32),
            pltpu.VMEM((8, width), jnp.float32),
        ),
        in_specs=[
            pl.BlockSpec(memory_space=pl.ANY),
            pl.BlockSpec(memory_space=pltpu.HBM),
            pl.BlockSpec(memory_space=pltpu.HBM),
        ],
        out_specs=(pl.BlockSpec(memory_space=pltpu.VMEM), pl.BlockSpec(memory_space=pltpu.VMEM)),
        scratch_shapes=[
            pltpu.VMEM((steps_k, width, paths), jnp.bfloat16),
            pltpu.VMEM((128, 128), jnp.int32),
            pltpu.VMEM((128, 128), jnp.int32),
            pltpu.VMEM((width, paths), jnp.float32),
            pltpu.VMEM((3, 1024, paths), jnp.bfloat16),
            pltpu.VMEM((steps_k, 16, paths), jnp.bfloat16),
            pltpu.VMEM((steps_k, 1024), jnp.float32),
            pltpu.VMEM((2, 64, 4, 128), jnp.float32),
            pltpu.VMEM((2, 32, 4, 128), jnp.float32),
            pltpu.VMEM((2, 32, 4, 128), jnp.float32),
            pltpu.VMEM((2, 64, 4, 128), jnp.float32),
            pltpu.VMEM((64, 4, 128), jnp.float32),
            pltpu.VMEM((2, 4, 128), jnp.float32),
            pltpu.VMEM((16, 4, 128), jnp.float32),
            pltpu.SemaphoreType.DMA((2,)),
            pltpu.SemaphoreType.DMA((steps_k,)),
            pltpu.SemaphoreType.DMA((2,)),
            pltpu.SemaphoreType.DMA((2,)),
            pltpu.SemaphoreType.DMA((2,)),
            pltpu.SemaphoreType.DMA((2,)),
            pltpu.SemaphoreType.DMA((2,)),
            pltpu.SemaphoreType.DMA((2,)),
        ],
        compiler_params=pltpu.CompilerParams(
            collective_id=0, has_side_effects=True, vmem_limit_bytes=67043328 - 64 * 1024
        ),
    )(slabs, level_table.reshape(128, 128), time_table.reshape(128, 128))
    return (value.reshape(8), grad)


def solution(mesh):
    placed = (P(("path", "tm"), None, None), P(), P())
    return jax.shard_map(
        shards, mesh=mesh, in_specs=placed, out_specs=(P("tm"), P("tm", None)), check_vma=False
    )
```
